128 devices in a mesh: expert: 32 (over z, y, core), dp: 4 (over x).
Axes of the slice: x: 4, y: 4, z: 4, core: 2. Of those that a mesh axis runs over, the one named last changes fastest.
Arguments:
- tokens: bfloat16 [2, 8192, 1024], P(None, ('expert', 'dp')), may hold values from -6 to 6
- routes: int32 [2, 8192, 6], P(None, ('expert', 'dp')), may hold values from 0 to 31, all different within a row; in each aligned block of 64 rows (0 to 63, 64 to 127, ..., all dimensions but the last counted through in order) at most 16 rows name the same one
- gate_weights: float32 [2, 8192, 6], P(None, ('expert', 'dp')), may hold values from 0.05 to 0.35
- cotangent: bfloat16 [2, 8192, 1024], P(None, ('expert', 'dp')), may hold values from -6 to 6
- expert_plan: int32 [32], replicated, may hold values from 0 to 31, each once
- weight_in: bfloat16 [32, 1024, 1536], P('expert', 'dp'), may hold values from -0.1875 to 0.1875
- weight_out: bfloat16 [32, 768, 1024], P('expert', 'dp'), may hold values from -0.21875 to 0.21875
- first_in: float32 [32, 1024, 1536], P('expert', 'dp'), may hold values from -6 to 6
- second_in: float32 [32, 1024, 1536], P('expert', 'dp'), may hold values from 0.5 to 20
- first_out: float32 [32, 768, 1024], P('expert', 'dp'), may hold values from -6 to 6
- second_out: float32 [32, 768, 1024], P('expert', 'dp'), may hold values from 0.5 to 20
Outputs:
- layer_output: bfloat16 [2, 8192, 1024], P(None, ('expert', 'dp'))
- token_gradient: bfloat16 [2, 8192, 1024], P(None, ('expert', 'dp'))
- weight_in_next: bfloat16 [32, 1024, 1536], P('expert', 'dp')
- weight_out_next: bfloat16 [32, 768, 1024], P('expert', 'dp')
- first_in_next: float32 [32, 1024, 1536], P('expert', 'dp')
- second_in_next: float32 [32, 1024, 1536], P('expert', 'dp')
- first_out_next: float32 [32, 768, 1024], P('expert', 'dp')
- second_out_next: float32 [32, 768, 1024], P('expert', 'dp')
The draws below stay inside these ranges and needn't reach their ends.
Inputs may be any that keep to these rules, and one draw needn't show every extreme that they name: `routes`: each row names 6 different experts. In the 64 rows of one device in one micro-batch (an aligned block), no expert is named by more than 16 rows; in some blocks one expert is named by exactly 16 rows. A permutation. Before the migration, index d of the expert axis holds expert d; after it, expert expert_plan[d].
All inputs are finite; a program needn't handle non-finite values.
Results may differ from the reference program's by a relative error of at most 0.014.
Values may be sent and summed in bfloat16 or wider, within the bound.
No kernel may reach another device: no remote copies, remote signals or barrier semaphores. Data moves between devices by JAX's collectives and lax.ppermute only.
A program may use at most 128 MiB of HBM per device.

```python
import math
import jax
import jax.numpy as jnp
import numpy as np
from jax import lax

D = 1024
FF = 768
TOP = 6
MICRO = 2
TOK_MB = 64
EXPERTS = 32
CAP = 16
TOKENS = 8192
N_EXPERT = 32
N_DP = 4


def level_of(own_key, shape, split, smallest, top_value):
    def one(axis_at, blocks):
        steps = jax.random.uniform(jax.random.fold_in(jax.random.fold_in(own_key, 6), axis_at), (blocks,), jnp.float32, smallest / len(split), top_value / len(split))
        return jnp.repeat(jnp.exp(steps), shape[axis_at] // blocks).reshape((-1,) + (1,) * (len(shape) - axis_at - 1))

    gain = one(*split[0])
    for cut in split[1:]:
        gain = gain * one(*cut)
    return gain


def shared_out(rng, own, number, rows, amount, top, reach, slope):
    ranking = jax.random.permutation(rng, amount)
    crowded, ordinary = portions_of(amount, rows * top, reach, slope, True), portions_of(amount, rows * top, reach, slope, False)
    places = jnp.arange(amount)

    def named(lengths, turn):
        used = int((lengths > 0).sum())
        fixed = max(1, used // 4)
        passed = fixed + (places - fixed + turn * (used - fixed)) % max(1, amount - fixed)
        return jnp.zeros((amount,), jnp.int32).at[ranking[jnp.where(places < fixed, places, passed)]].set(jnp.asarray(lengths, jnp.int32))

    lengths = jnp.where(number % 4 == 0, named(crowded, number // 4), named(ordinary, number - number // 4 - 1))
    mixed = jax.random.permutation(jax.random.fold_in(own, 3), amount)
    source_of, sink = mixed[0:amount // 2 * 2:2], mixed[1:amount // 2 * 2:2]
    room = jnp.minimum(lengths[source_of] - 1, reach - lengths[sink]) // 2
    room = jnp.where((source_of == ranking[0]) | (sink == ranking[0]) | (lengths[sink] == 0), 0, jnp.maximum(room, 0))
    passed = jax.random.randint(jax.random.fold_in(own, 4), (amount // 2,), 0, 1 << 20) % (room + 1)
    lengths = lengths.at[source_of].add(-passed).at[sink].add(passed)
    members = jnp.searchsorted(jnp.cumsum(lengths), jnp.arange(rows * top), side="right").astype(jnp.int32)
    listing = members.reshape(top, rows).T
    listing = listing[jax.random.permutation(jax.random.fold_in(own, 1), rows)]
    turn = jax.random.randint(jax.random.fold_in(own, 2), (rows, 1), 0, top)
    return jnp.take_along_axis(listing, (jnp.arange(top)[None, :] + turn) % top, axis=1)


def portions_of(amount, total, most, skew, full):
    loads = [(1 << 20) // math.isqrt(standing ** skew) + 1 for standing in range(1, amount + 1)]
    largest = most if full else min(most, max(-(-total // amount), total * loads[0] // sum(loads)))
    least = 1 if total - largest >= amount - 1 else 0
    given, surplus = [largest] + [least] * (amount - 1), total - largest - least * (amount - 1)
    while surplus > 0:
        free = [i for i in range(1, amount) if given[i] < largest] or [i for i in range(1, amount) if given[i] < most]
        pool, budget = sum([loads[i] for i in free]), surplus
        for i in free:
            addition = min(most - given[i], max(1, budget * loads[i] // pool), surplus)
            given[i] = given[i] + addition
            surplus = surplus - addition
    return np.array(given)


def centred(rng, dims, scale, most, cuts=(), kind=jnp.bfloat16):
    array = jax.random.normal(rng, dims, jnp.float32) * scale
    if len(cuts) > 0:
        array = level_of(rng, dims, cuts, -0.22, 0.18) * array
    return jnp.clip(array, min=-most, max=most).astype(kind)


def setup_inputs(seed: int = 0) -> dict:
    key_of = jax.random.split(jax.random.key(seed), 12)
    tokens = centred(key_of[0], (MICRO, TOKENS, D), 1.0, 6.0, ((1, 128),))
    routes_keys = jax.random.split(jax.random.fold_in(key_of[1], 1), MICRO * TOKENS // TOK_MB)
    routes_turns = jax.random.permutation(jax.random.fold_in(key_of[1], 3), MICRO * TOKENS // TOK_MB)
    routes = jax.vmap(lambda own, number: shared_out(jax.random.fold_in(key_of[1], 2), own, number, TOK_MB, EXPERTS, TOP, CAP, 2))(routes_keys, routes_turns).reshape((MICRO, TOKENS, TOP))
    gate_weights = jnp.clip(0.05 + 0.29999999 * jax.random.uniform(key_of[2], (MICRO, TOKENS, TOP), jnp.float32) ** level_of(key_of[2], (MICRO, TOKENS, TOP), ((1, 128),), -0.2, 0.2), 0.05, 0.35)
    cotangent = centred(key_of[3], (MICRO, TOKENS, D), 1.0, 6.0, ((1, 128),))
    expert_plan = jax.random.permutation(key_of[4], EXPERTS).astype(jnp.int32)
    weight_in = centred(key_of[5], (EXPERTS, D, 2 * FF), D ** -0.5, 0.1875, ((0, 32), (1, 4)))
    weight_out = centred(key_of[6], (EXPERTS, FF, D), FF ** -0.5, 0.21875, ((0, 32), (1, 4)))
    first_in = centred(key_of[7], (EXPERTS, D, 2 * FF), 1.0, 6.0, ((0, 32), (1, 4)), jnp.float32)
    second_in = jnp.clip(jnp.exp(math.log(20.0) - 3.6888795 * jax.random.uniform(key_of[8], (EXPERTS, D, 2 * FF), jnp.float32) ** level_of(key_of[8], (EXPERTS, D, 2 * FF), ((0, 32), (1, 4)), -0.2, 0.2)), 0.5, 20.0)
    first_out = centred(key_of[9], (EXPERTS, FF, D), 1.0, 6.0, ((0, 32), (1, 4)), jnp.float32)
    second_out = jnp.clip(jnp.exp(math.log(20.0) - 3.6888795 * jax.random.uniform(key_of[10], (EXPERTS, FF, D), jnp.float32) ** level_of(key_of[10], (EXPERTS, FF, D), ((0, 32), (1, 4)), -0.2, 0.2)), 0.5, 20.0)
    return {"tokens": tokens, "routes": routes, "gate_weights": gate_weights, "cotangent": cotangent, "expert_plan": expert_plan, "weight_in": weight_in, "weight_out": weight_out, "first_in": first_in, "second_in": second_in, "first_out": first_out, "second_out": second_out}


beta_one = 0.9
beta_two = 0.95
learn_rate = 0.00042
decay_rate = 0.1
epsilon = 1e-08
steps_done = 10

def slot_ranks(chosen):
    hits = (chosen[..., None] == jnp.arange(EXPERTS, dtype=jnp.int32)).astype(jnp.int32)
    per_token = lax.optimization_barrier(jnp.sum(hits, axis=3))
    before = jnp.cumsum(per_token, axis=2) - per_token
    return lax.optimization_barrier(jnp.sum(hits * before[:, :, :, None, :], axis=4)).astype(jnp.int32)

def expert_pass(rows, grads, weight_first, weight_second):
    pre = jnp.dot(rows, weight_first, preferred_element_type=jnp.float32)
    gate_part = pre[:, :FF]
    up_part = pre[:, FF:]
    sigma = jax.nn.sigmoid(gate_part)
    hidden = (gate_part * sigma * up_part).astype(jnp.bfloat16)
    output = jnp.dot(hidden, weight_second, preferred_element_type=jnp.float32).astype(jnp.bfloat16)
    hidden_grad = lax.dot_general(grads, weight_second, (((1,), (1,)), ((), ())), preferred_element_type=jnp.float32)
    pre_grad = jnp.concatenate([hidden_grad * up_part * sigma * (1.0 + gate_part * (1.0 - sigma)), hidden_grad * gate_part * sigma], axis=1).astype(jnp.bfloat16)
    grad_first = lax.dot_general(rows, pre_grad, (((0,), (0,)), ((), ())), preferred_element_type=jnp.float32)
    grad_second = lax.dot_general(hidden, grads, (((0,), (0,)), ((), ())), preferred_element_type=jnp.float32)
    token_part = lax.dot_general(pre_grad, weight_first, (((1,), (1,)), ((), ())), preferred_element_type=jnp.float32).astype(jnp.bfloat16)
    return (output, token_part, grad_first, grad_second)

def adam_update(weight, gradient, first, second):
    first_new = beta_one * first + (1.0 - beta_one) * gradient
    second_new = beta_two * second + (1.0 - beta_two) * gradient * gradient
    ratio = first_new / (1.0 - beta_one ** steps_done) / (jnp.sqrt(second_new / (1.0 - beta_two ** steps_done)) + epsilon)
    master = weight.astype(jnp.float32)
    return ((master - learn_rate * (ratio + decay_rate * master)).astype(jnp.bfloat16), first_new, second_new)

def reference(tokens, routes, gate_weights, cotangent, expert_plan, weight_in, weight_out, first_in, second_in, first_out, second_out):
    blocks = N_EXPERT * N_DP
    inputs = tokens.reshape(MICRO, blocks, TOK_MB, D)
    chosen = routes.reshape(MICRO, blocks, TOK_MB, TOP)
    gates = gate_weights.reshape(MICRO, blocks, TOK_MB, TOP)
    upstream = cotangent.reshape(MICRO, blocks, TOK_MB, D)
    ranks = slot_ranks(chosen)
    micro_index = jnp.broadcast_to(jnp.arange(MICRO, dtype=jnp.int32)[:, None, None, None], chosen.shape)
    block_index = jnp.broadcast_to(jnp.arange(blocks, dtype=jnp.int32)[None, :, None, None], chosen.shape)
    spread = jnp.broadcast_to(inputs[:, :, :, None, :], chosen.shape + (D,))
    sent = jnp.zeros((EXPERTS, MICRO, blocks, CAP, D), jnp.bfloat16).at[chosen, micro_index, block_index, ranks].set(spread)
    scaled = (gates[..., None] * upstream[:, :, :, None, :].astype(jnp.float32)).astype(jnp.bfloat16)
    sent_grad = jnp.zeros((EXPERTS, MICRO, blocks, CAP, D), jnp.bfloat16).at[chosen, micro_index, block_index, ranks].set(scaled)

    def per_expert(expert):
        rows = sent[expert].reshape(MICRO, N_EXPERT, N_DP, CAP, D)
        grads = sent_grad[expert].reshape(MICRO, N_EXPERT, N_DP, CAP, D)
        weight_first = weight_in[expert]
        weight_second = weight_out[expert]
        outputs = []
        backs = []
        total_first = jnp.zeros((D, 2 * FF), jnp.float32)
        total_second = jnp.zeros((FF, D), jnp.float32)
        for replica in range(N_DP):
            mine = rows[:, :, replica].reshape(-1, D)
            mine_grad = grads[:, :, replica].reshape(-1, D)
            output, token_part, grad_first, grad_second = expert_pass(mine, mine_grad, weight_first, weight_second)
            outputs.append(output.reshape(MICRO, N_EXPERT, CAP, D))
            backs.append(token_part.reshape(MICRO, N_EXPERT, CAP, D))
            total_first = total_first + lax.optimization_barrier(grad_first.astype(jnp.bfloat16)).astype(jnp.float32)
            total_second = total_second + lax.optimization_barrier(grad_second.astype(jnp.bfloat16)).astype(jnp.float32)
        outputs = jnp.stack(outputs, axis=2).reshape(MICRO, blocks, CAP, D)
        backs = jnp.stack(backs, axis=2).reshape(MICRO, blocks, CAP, D)
        return (outputs, backs, total_first, total_second)
    outputs, backs, grad_in, grad_out = lax.map(per_expert, jnp.arange(EXPERTS, dtype=jnp.int32))
    picked = outputs[chosen, micro_index, block_index, ranks]
    layer_output = lax.optimization_barrier(jnp.sum(gates[..., None] * picked.astype(jnp.float32), axis=3)).astype(jnp.bfloat16).reshape(MICRO, TOKENS, D)
    picked_grad = backs[chosen, micro_index, block_index, ranks]
    token_gradient = lax.optimization_barrier(jnp.sum(picked_grad.astype(jnp.float32), axis=3)).astype(jnp.bfloat16).reshape(MICRO, TOKENS, D)
    new_in, first_in_new, second_in_new = adam_update(weight_in, grad_in, first_in, second_in)
    new_out, first_out_new, second_out_new = adam_update(weight_out, grad_out, first_out, second_out)
    return (layer_output, token_gradient, jnp.take(new_in, expert_plan, axis=0), jnp.take(new_out, expert_plan, axis=0), jnp.take(first_in_new, expert_plan, axis=0), jnp.take(second_in_new, expert_plan, axis=0), jnp.take(first_out_new, expert_plan, axis=0), jnp.take(second_out_new, expert_plan, axis=0))
```

```python
import functools

import jax
import jax.numpy as jnp
from jax import lax
from jax.experimental import pallas as pl
from jax.experimental.pallas import tpu as pltpu
from jax.sharding import PartitionSpec as P

beta_one = 0.9
beta_two = 0.95
learn_rate = 0.00042
decay_rate = 0.1
epsilon = 1e-08
steps_done = 10

SIDE = 768
RI = 256
RO = 192
RT = 64
REP = 4
COUNT = 32
CAP = 16
ROWS = 2 * CAP

f32 = jnp.float32
bf16 = jnp.bfloat16
VMEM = pl.BlockSpec(memory_space=pltpu.VMEM)
SMEM = pl.BlockSpec(memory_space=pltpu.SMEM)
ANY = pl.BlockSpec(memory_space=pl.ANY)


def exchange(x):
    return lax.all_to_all(x, "expert", split_axis=0, concat_axis=0, tiled=True)


def shifted(x, by):
    return lax.ppermute(x, "dp", [(i, (i + by) % REP) for i in range(REP)])


def pack_body(w_in, w_out, f_in, f_out, s_in, s_out, out):
    for j, (a, b) in enumerate(((w_in, w_out), (f_in, f_out), (s_in, s_out))):
        lanes = slice(j * SIDE, (j + 1) * SIDE)
        out[0:RI, lanes] = a[:, :SIDE].astype(bf16)
        out[RI : 2 * RI, lanes] = a[:, SIDE:].astype(bf16)
        out[2 * RI : 2 * RI + RO, lanes] = b[:, :SIDE].astype(bf16)
        for i in range(3):
            at = j * SIDE + 256 * i
            out[2 * RI + RO :, at : at + 256] = b[RT * i : RT * i + RT, SIDE:].astype(bf16)


def pack(w_in, w_out, f_in, f_out, s_in, s_out):
    return pl.pallas_call(
        pack_body,
        out_shape=jax.ShapeDtypeStruct((SIDE, 3 * SIDE), bf16),
        in_specs=[VMEM] * 6,
        out_specs=VMEM,
        name="pack",
    )(w_in, w_out, f_in, f_out, s_in, s_out)


def pick_body(lo, size, plan, src, out, sem):
    copies = [
        pltpu.make_async_copy(src.at[plan[d], :, lo : lo + size], out.at[d], sem.at[d]) for d in range(COUNT)
    ]
    for c in copies:
        c.start()
    for c in copies:
        c.wait()


def pick(plan, src, lo, size):
    return pl.pallas_call(
        functools.partial(pick_body, lo, size),
        out_shape=jax.ShapeDtypeStruct((COUNT, SIDE // COUNT, size), bf16),
        in_specs=[SMEM, ANY],
        out_specs=ANY,
        scratch_shapes=[pltpu.SemaphoreType.DMA((COUNT,))],
        name="pick",
    )(plan, src)


def dispatch_body(routes, gates, plan, tokens, cotangent, out, place, gated):
    n = tokens.shape[1]
    top = routes.shape[0]
    holder = plan[...]
    earlier = (
        lax.broadcasted_iota(jnp.int32, (n, n), 0) < lax.broadcasted_iota(jnp.int32, (n, n), 1)
    ).astype(bf16)
    slot = lax.broadcasted_iota(jnp.int32, (COUNT, CAP, n), 1).astype(f32)
    for m in range(2):
        hit = jnp.zeros((COUNT, n), f32)
        gate = jnp.zeros((COUNT, n), f32)
        for k in range(top):
            one = routes[k, m : m + 1, :] == holder
            hit = hit + jnp.where(one, 1.0, 0.0)
            gate = gate + jnp.where(one, gates[k, m : m + 1, :], 0.0)
        rank = jnp.dot(hit.astype(bf16), earlier, preferred_element_type=f32)
        rank = jnp.where(hit > 0.0, rank, -1.0)
        wide = jnp.broadcast_to(rank[:, None, :], (COUNT, CAP, n))
        chosen = jnp.where(wide == slot, 1.0, 0.0)
        weighted = chosen * jnp.broadcast_to(gate[:, None, :], (COUNT, CAP, n))
        chosen = chosen.reshape(COUNT * CAP, n)
        weighted = weighted.reshape(COUNT * CAP, n)
        column = jnp.sum(weighted, axis=1, keepdims=True)
        chosen = chosen.astype(bf16)
        high = weighted.astype(bf16)
        low = (weighted - high.astype(f32)).astype(bf16)
        place[m] = chosen
        gated[m, :, :n] = high
        gated[m, :, n:] = low
        sent = jnp.dot(chosen, tokens[m], preferred_element_type=f32).astype(bf16)
        out[:, CAP * m : CAP * m + CAP, :] = sent.reshape(COUNT, CAP, -1)
        grads = jnp.dot(chosen, cotangent[m], preferred_element_type=f32) * column
        out[:, ROWS + CAP * m : ROWS + CAP * m + CAP, :] = grads.astype(bf16).reshape(COUNT, CAP, -1)


def dispatch(routes, gates, plan, tokens, cotangent):
    n, width = tokens.shape[1:]
    return pl.pallas_call(
        dispatch_body,
        out_shape=(
            jax.ShapeDtypeStruct((COUNT, 2 * ROWS, width), bf16),
            jax.ShapeDtypeStruct((2, COUNT * CAP, n), bf16),
            jax.ShapeDtypeStruct((2, COUNT * CAP, 2 * n), bf16),
        ),
        in_specs=[VMEM] * 5,
        out_specs=(VMEM, VMEM, VMEM),
        name="dispatch",
    )(routes, gates, plan, tokens, cotangent)


ROW_T = (((0,), (0,)), ((), ()))
COL_T = (((1,), (1,)), ((), ()))


def combine_body(back, place, gated, layer, token):
    n = layer.shape[1]
    for m in range(2):
        rows = back[:, CAP * m : CAP * m + CAP, :].reshape(COUNT * CAP, -1)
        both = lax.dot_general(gated[m], rows, ROW_T, preferred_element_type=f32)
        layer[m] = (both[:n] + both[n:]).astype(bf16)
        rows = back[:, ROWS + CAP * m : ROWS + CAP * m + CAP, :].reshape(COUNT * CAP, -1)
        token[m] = lax.dot_general(place[m], rows, ROW_T, preferred_element_type=f32).astype(bf16)


def combine(back, place, gated):
    n = place.shape[2]
    width = back.shape[2]
    shape = jax.ShapeDtypeStruct((2, n, width), bf16)
    return pl.pallas_call(
        combine_body,
        out_shape=(shape, shape),
        in_specs=[VMEM] * 3,
        out_specs=(VMEM, VMEM),
        name="combine",
    )(back, place, gated)


def expert_body(mine, rows, w0, w1, w2, w3, back, g0, g1, g2, g3, win, wout, hid, pgrad, gout, gpack, sem, gsem):
    r = mine[0]
    copies = []
    for s, w in enumerate((w0, w1, w2, w3)):
        q = (r - s + REP) % REP
        at = pl.multiple_of(q * RI, RI)
        to = pl.multiple_of(q * RO, RT)
        pieces = [
            (w.at[0:RI], win.at[pl.ds(at, RI), 0:SIDE]),
            (w.at[RI : 2 * RI], win.at[pl.ds(at, RI), SIDE : 2 * SIDE]),
            (w.at[2 * RI : 2 * RI + RO], wout.at[pl.ds(to, RO), 0:SIDE]),
        ]
        for i in range(3):
            pieces.append(
                (
                    w.at[2 * RI + RO : SIDE, 256 * i : 256 * i + 256],
                    wout.at[pl.ds(to + RT * i, RT), SIDE : SIDE + 256],
                )
            )
        for a, b in pieces:
            copies.append(pltpu.make_async_copy(a, b, sem.at[len(copies)]))
    for c in copies:
        c.start()
    for c in copies:
        c.wait()

    group = 8
    size = group * ROWS

    def step(i, carry):
        own = pl.ds(pl.multiple_of(i * group, group), group)
        at = pl.ds(pl.multiple_of(i * size, size), size)
        x = rows[own, 0:ROWS, :].reshape(size, -1)
        pre = jnp.dot(x, win[...], preferred_element_type=f32)
        gate = pre[:, :SIDE]
        up = pre[:, SIDE:]
        sigma = jax.nn.sigmoid(gate)
        swish = gate * sigma
        hidden = (swish * up).astype(bf16)
        hid[at, :] = hidden
        out = jnp.dot(hidden, wout[...], preferred_element_type=f32).astype(bf16)
        back[own, 0:ROWS, :] = out.reshape(group, ROWS, -1)
        g = rows[own, ROWS : 2 * ROWS, :].reshape(size, -1)
        hgrad = lax.dot_general(g, wout[...], COL_T, preferred_element_type=f32)
        pgrad[at, 0:SIDE] = (hgrad * up * sigma * (1.0 + gate * (1.0 - sigma))).astype(bf16)
        pgrad[at, SIDE:] = (hgrad * swish).astype(bf16)
        part = lax.dot_general(pgrad[at, :], win[...], COL_T, preferred_element_type=f32).astype(bf16)
        back[own, ROWS : 2 * ROWS, :] = part.reshape(group, ROWS, -1)
        return carry

    lax.fori_loop(0, COUNT // group, step, 0)
    for q in range(REP):
        x = rows[:, 0:ROWS, RI * q : RI * q + RI].reshape(COUNT * ROWS, RI)
        grad = lax.dot_general(x, pgrad[...], ROW_T, preferred_element_type=f32).astype(bf16)
        gpack[q, 0:RI, :] = grad[:, :SIDE]
        gpack[q, RI : 2 * RI, :] = grad[:, SIDE:]
    g = rows[:, ROWS : 2 * ROWS, :].reshape(COUNT * ROWS, -1)
    for j in range(3):
        gout[256 * j : 256 * j + 256, :] = lax.dot_general(
            hid[:, 256 * j : 256 * j + 256], g, ROW_T, preferred_element_type=f32
        ).astype(bf16)
    for q in range(REP):
        gpack[q, 2 * RI : 2 * RI + RO, :] = gout[RO * q : RO * q + RO, :SIDE]
        for i in range(3):
            gpack[q, 2 * RI + RO :, 256 * i : 256 * i + 256] = gout[RO * q + RT * i : RO * q + RT * i + RT, SIDE:]
    copies = [
        pltpu.make_async_copy(gpack.at[(r + s) % REP], out, gsem.at[s]) for s, out in enumerate((g0, g1, g2, g3))
    ]
    for c in copies:
        c.start()
    for c in copies:
        c.wait()


def expert(mine, rows, parts):
    width = rows.shape[2]
    piece = jax.ShapeDtypeStruct((SIDE, SIDE), bf16)
    total = COUNT * ROWS
    return pl.pallas_call(
        expert_body,
        out_shape=(jax.ShapeDtypeStruct(rows.shape, bf16), piece, piece, piece, piece),
        in_specs=[SMEM, VMEM, ANY, ANY, ANY, ANY],
        out_specs=(VMEM, ANY, ANY, ANY, ANY),
        scratch_shapes=[
            pltpu.VMEM((REP * RI, 2 * SIDE), bf16),
            pltpu.VMEM((REP * RO, width), bf16),
            pltpu.VMEM((total, SIDE), bf16),
            pltpu.VMEM((total, 2 * SIDE), bf16),
            pltpu.VMEM((SIDE, width), bf16),
            pltpu.VMEM((REP, SIDE, SIDE), bf16),
            pltpu.SemaphoreType.DMA((24,)),
            pltpu.SemaphoreType.DMA((REP,)),
        ],
        cost_estimate=pl.CostEstimate(flops=14_500_000_000, bytes_accessed=18_000_000, transcendentals=800_000),
        name="expert",
    )(mine, rows, *parts)


def adam(weight, gradient, first, second):
    first_new = beta_one * first + (1.0 - beta_one) * gradient
    second_new = beta_two * second + (1.0 - beta_two) * gradient * gradient
    ratio = (
        first_new
        / (1.0 - beta_one**steps_done)
        / (jnp.sqrt(second_new / (1.0 - beta_two**steps_done)) + epsilon)
    )
    master = weight.astype(f32)
    return (
        (master - learn_rate * (ratio + decay_rate * master)).astype(bf16),
        first_new,
        second_new,
    )


def update_body(w, moments, g0, g1, g2, g3, w_in, w_out, f_in, s_in, f_out, s_out):
    def one(rows, lanes, outs, at, to):
        grad = g0[rows, lanes].astype(f32)
        for g in (g1, g2, g3):
            grad = grad + g[rows, lanes].astype(f32)
        second = slice(lanes.start + SIDE, lanes.stop + SIDE)
        new = adam(w[rows, lanes], grad, moments[rows, lanes].astype(f32), moments[rows, second].astype(f32))
        for o, v in zip(outs, new):
            o[at, to] = v

    ins = (w_in, f_in, s_in)
    outs = (w_out, f_out, s_out)
    whole = slice(0, SIDE)
    for i in range(RI // RT):
        here = slice(RT * i, RT * i + RT)
        one(here, whole, ins, here, whole)
        one(slice(RI + RT * i, RI + RT * i + RT), whole, ins, here, slice(SIDE, 2 * SIDE))
    for i in range(3):
        here = slice(RT * i, RT * i + RT)
        one(slice(2 * RI + RT * i, 2 * RI + RT * i + RT), whole, outs, here, whole)
        one(slice(2 * RI + RO, SIDE), slice(256 * i, 256 * i + 256), outs, here, slice(SIDE, SIDE + 256))


def update(w, moments, grads):
    return pl.pallas_call(
        update_body,
        out_shape=(
            jax.ShapeDtypeStruct((RI, 2 * SIDE), bf16),
            jax.ShapeDtypeStruct((RO, 1024), bf16),
            jax.ShapeDtypeStruct((RI, 2 * SIDE), f32),
            jax.ShapeDtypeStruct((RI, 2 * SIDE), f32),
            jax.ShapeDtypeStruct((RO, 1024), f32),
            jax.ShapeDtypeStruct((RO, 1024), f32),
        ),
        in_specs=[VMEM] * 6,
        out_specs=(VMEM,) * 6,
        name="update",
    )(w, moments, *grads)


def on_device(
    tokens,
    routes,
    gate_weights,
    cotangent,
    expert_plan,
    weight_in,
    weight_out,
    first_in,
    second_in,
    first_out,
    second_out,
):
    mine = lax.axis_index("dp").astype(jnp.int32).reshape(1)
    packed = pack(weight_in[0], weight_out[0], first_in[0], first_out[0], second_in[0], second_out[0])
    spread = exchange(packed.reshape(COUNT, SIDE // COUNT, 3 * SIDE))
    own = exchange(pick(expert_plan, spread, 0, SIDE)).reshape(SIDE, SIDE)
    outgoing, place, gated = dispatch(
        routes.transpose(2, 0, 1), gate_weights.transpose(2, 0, 1), expert_plan.reshape(-1, 1), tokens, cotangent
    )
    outgoing, own = lax.optimization_barrier((outgoing, own))
    parts = (own, shifted(own, 1), shifted(own, 2), shifted(own, 3))
    arrived = exchange(outgoing)
    moved = pick(expert_plan, spread, SIDE, 2 * SIDE)
    arrived, moved = lax.optimization_barrier((arrived, moved))
    moments = exchange(moved).reshape(SIDE, 2 * SIDE)
    back, g0, g1, g2, g3 = expert(mine, arrived, parts)
    back, moments = lax.optimization_barrier((back, moments))
    grads = (g0, shifted(g1, 1), shifted(g2, 2), shifted(g3, 3))
    returned = exchange(back)
    new_in, new_out, first_in_new, second_in_new, first_out_new, second_out_new = update(own, moments, grads)
    layer, token = combine(returned, place, gated)
    return (
        layer,
        token,
        new_in[None],
        new_out[None],
        first_in_new[None],
        second_in_new[None],
        first_out_new[None],
        second_out_new[None],
    )


def solution(mesh):
    rows = P(None, ("expert", "dp"), None)
    held = P("expert", "dp", None)
    return jax.shard_map(
        on_device,
        mesh=mesh,
        in_specs=(rows,) * 4 + (P(),) + (held,) * 6,
        out_specs=(rows,) * 2 + (held,) * 6,
        check_vma=False,
    )
```

```python
import jax
import jax.numpy as jnp
from jax import lax
from jax.experimental import pallas as pl
from jax.experimental.pallas import tpu as pltpu
from jax.sharding import PartitionSpec as P


beta_one = 0.9
beta_two = 0.95
learn_rate = 0.00042
decay_rate = 0.1
epsilon = 1e-08
steps_done = 10

SIDE = 768
RI = 256
RO = 192
RT = 64
REP = 4
COUNT = 32
CAP = 16
ROWS = 2 * CAP
HALF = SIDE // 2
CHUNKS = 2

f32 = jnp.float32
bf16 = jnp.bfloat16
VMEM = pl.BlockSpec(memory_space=pltpu.VMEM)
SMEM = pl.BlockSpec(memory_space=pltpu.SMEM)
ANY = pl.BlockSpec(memory_space=pl.ANY)


ROW_T = (((0,), (0,)), ((), ()))
COL_T = (((1,), (1,)), ((), ()))


def exchange(x):
    return lax.all_to_all(x, "expert", split_axis=0, concat_axis=0, tiled=True)


def shifted(x, by):
    return lax.ppermute(x, "dp", [(i, (i + by) % REP) for i in range(REP)])


def both(a, b):
    return (a.astype(f32) + b.astype(f32)).astype(bf16)


def pack_body(w_in, w_out, f_in, f_out, s_in, s_out, out):
    for j, (a, b) in enumerate(((f_in, f_out), (s_in, s_out), (w_in, w_out))):
        lanes = slice(j * SIDE, (j + 1) * SIDE)
        out[0:RI, lanes] = a[:, :SIDE].astype(bf16)
        out[RI : 2 * RI, lanes] = a[:, SIDE:].astype(bf16)
        out[2 * RI : 2 * RI + RO, lanes] = b[:, :SIDE].astype(bf16)
        for i in range(3):
            at = j * SIDE + 256 * i
            out[2 * RI + RO :, at : at + 256] = b[RT * i : RT * i + RT, SIDE:].astype(bf16)


def pack(w_in, w_out, f_in, f_out, s_in, s_out):
    return pl.pallas_call(
        pack_body,
        out_shape=jax.ShapeDtypeStruct((SIDE, 3 * SIDE), bf16),
        in_specs=[VMEM] * 6,
        out_specs=VMEM,
        name="pack",
    )(w_in, w_out, f_in, f_out, s_in, s_out)


def pick_body(plan, src, out):
    def step(d, carry):
        out[d] = src[plan[d]]
        return carry

    lax.fori_loop(0, COUNT, step, 0, unroll=True)


def pick(plan, src, lo, size):
    shape = (COUNT, SIDE // COUNT, size)
    return pl.pallas_call(
        pick_body,
        grid=(1,),
        out_shape=jax.ShapeDtypeStruct(shape, bf16),
        in_specs=[SMEM, pl.BlockSpec(shape, lambda i: (0, 0, lo // size))],
        out_specs=pl.BlockSpec(shape, lambda i: (0, 0, 0)),
        name="pick",
    )(plan, src)


def dispatch_body(routes, gates, plan, tokens, cotangent, out, place, gated):
    n = tokens.shape[1]
    top = routes.shape[0]
    holder = plan[...]
    earlier = (
        lax.broadcasted_iota(jnp.int32, (n, n), 0) < lax.broadcasted_iota(jnp.int32, (n, n), 1)
    ).astype(bf16)
    same = (
        lax.broadcasted_iota(jnp.int32, (n, n), 0) == lax.broadcasted_iota(jnp.int32, (n, n), 1)
    ).astype(bf16)
    slot = lax.broadcasted_iota(jnp.int32, (COUNT, CAP, n), 1).astype(f32)
    for m in range(2):
        hit = jnp.zeros((COUNT, n), f32)
        gate = jnp.zeros((COUNT, n), f32)
        for k in range(top):
            one = routes[k, m : m + 1, :] == holder
            hit = hit + jnp.where(one, 1.0, 0.0)
            gate = gate + jnp.where(one, gates[k, m : m + 1, :], 0.0)
        rank = jnp.dot(hit.astype(bf16), earlier, preferred_element_type=f32)
        rank = jnp.where(hit > 0.0, rank, -1.0)
        wide = jnp.broadcast_to(rank[:, None, :], (COUNT, CAP, n))
        chosen = jnp.where(wide == slot, 1.0, 0.0)
        weighted = chosen * jnp.broadcast_to(gate[:, None, :], (COUNT, CAP, n))
        chosen = chosen.reshape(COUNT * CAP, n)
        weighted = weighted.reshape(COUNT * CAP, n)
        column = jnp.sum(weighted, axis=1, keepdims=True)
        chosen = chosen.astype(bf16)
        high = weighted.astype(bf16)
        low = (weighted - high.astype(f32)).astype(bf16)
        place[m] = lax.dot_general(same, chosen, COL_T, preferred_element_type=f32).astype(bf16)
        gated[m, :n] = lax.dot_general(same, high, COL_T, preferred_element_type=f32).astype(bf16)
        gated[m, n:] = lax.dot_general(same, low, COL_T, preferred_element_type=f32).astype(bf16)
        sent = jnp.dot(chosen, tokens[m], preferred_element_type=f32).astype(bf16)
        out[:, CAP * m : CAP * m + CAP, :] = sent.reshape(COUNT, CAP, -1)
        grads = jnp.dot(chosen, cotangent[m], preferred_element_type=f32) * column
        out[:, ROWS + CAP * m : ROWS + CAP * m + CAP, :] = grads.astype(bf16).reshape(COUNT, CAP, -1)


def dispatch(routes, gates, plan, tokens, cotangent):
    n, width = tokens.shape[1:]
    return pl.pallas_call(
        dispatch_body,
        out_shape=(
            jax.ShapeDtypeStruct((COUNT, 2 * ROWS, width), bf16),
            jax.ShapeDtypeStruct((2, n, COUNT * CAP), bf16),
            jax.ShapeDtypeStruct((2, 2 * n, COUNT * CAP), bf16),
        ),
        in_specs=[VMEM] * 5,
        out_specs=(VMEM, VMEM, VMEM),
        name="dispatch",
    )(routes, gates, plan, tokens, cotangent)


def combine_body(back, place, gated, layer, token, buf, sem):
    n = layer.shape[1]
    size = COUNT // CHUNKS
    copies = [
        pltpu.make_async_copy(back.at[i * size : (i + 1) * size], buf.at[i], sem.at[i]) for i in range(CHUNKS)
    ]
    for c in copies:
        c.start()
    sums = [None] * 4
    for i, c in enumerate(copies):
        c.wait()
        slots = slice(i * size * CAP, (i + 1) * size * CAP)
        for m in range(2):
            for j, (table, at) in enumerate(((gated, 0), (place, ROWS))):
                rows = buf[i, :, at + CAP * m : at + CAP * m + CAP, :].reshape(size * CAP, -1)
                part = jnp.dot(table[m, :, slots], rows, preferred_element_type=f32)
                sums[2 * j + m] = part if i == 0 else sums[2 * j + m] + part
    for m in range(2):
        layer[m] = (sums[m][:n] + sums[m][n:]).astype(bf16)
        token[m] = sums[2 + m].astype(bf16)


def combine(back, place, gated):
    n = place.shape[1]
    width = back.shape[2]
    shape = jax.ShapeDtypeStruct((2, n, width), bf16)
    return pl.pallas_call(
        combine_body,
        out_shape=(shape, shape),
        in_specs=[ANY, VMEM, VMEM],
        out_specs=(VMEM, VMEM),
        scratch_shapes=[
            pltpu.VMEM((CHUNKS, COUNT // CHUNKS, 2 * ROWS, width), bf16),
            pltpu.SemaphoreType.DMA((CHUNKS,)),
        ],
        name="combine",
    )(back, place, gated)


def expert_body(mine, rows, w0, w1, w2a, w2b, w3, back, g0, g1t, g1b, g2t, g2b, g3t, g3b, win, wout, hid, pgrad, gout, gpack, sem, gsem):
    r = mine[0]
    copies = []

    def fetch(s, w, lo, hi, src):
        q = (r - s + REP) % REP
        at = pl.multiple_of(q * RI, RI)
        to = pl.multiple_of(q * RO, RT)
        pieces = []
        for base, end, ref, first, lanes in (
            (0, RI, win, at, 0),
            (RI, 2 * RI, win, at, SIDE),
            (2 * RI, 2 * RI + RO, wout, to, 0),
        ):
            l, h = max(lo, base), min(hi, end)
            if l < h:
                start = pl.multiple_of(first + (l - base), RT)
                pieces.append((w.at[l - lo + src : h - lo + src], ref.at[pl.ds(start, h - l), lanes : lanes + SIDE]))
        if hi == SIDE:
            for i in range(3):
                l = 2 * RI + RO - lo + src
                start = pl.multiple_of(to + RT * i, RT)
                pieces.append(
                    (w.at[l : l + RT, 256 * i : 256 * i + 256], wout.at[pl.ds(start, RT), SIDE : SIDE + 256])
                )
        for x, y in pieces:
            copies.append(pltpu.make_async_copy(x, y, sem.at[len(copies)]))

    fetch(0, w0, 0, SIDE, 0)
    fetch(1, w1, 0, SIDE, 0)
    fetch(2, w2a, 0, HALF, 0)
    fetch(2, w2b, HALF, SIDE, 0)
    fetch(3, w3, 0, SIDE, 0)
    for c in copies:
        c.start()
    for c in copies:
        c.wait()

    group = 8
    size = group * ROWS

    def step(i, carry):
        own = pl.ds(pl.multiple_of(i * group, group), group)
        at = pl.ds(pl.multiple_of(i * size, size), size)
        x = rows[own, 0:ROWS, :].reshape(size, -1)
        pre = jnp.dot(x, win[...], preferred_element_type=f32)
        gate = pre[:, :SIDE]
        up = pre[:, SIDE:]
        sigma = jax.nn.sigmoid(gate)
        swish = gate * sigma
        hidden = (swish * up).astype(bf16)
        hid[at, :] = hidden
        out = jnp.dot(hidden, wout[...], preferred_element_type=f32).astype(bf16)
        back[own, 0:ROWS, :] = out.reshape(group, ROWS, -1)
        g = rows[own, ROWS : 2 * ROWS, :].reshape(size, -1)
        hgrad = lax.dot_general(g, wout[...], COL_T, preferred_element_type=f32)
        pgrad[at, 0:SIDE] = (hgrad * up * sigma * (1.0 + gate * (1.0 - sigma))).astype(bf16)
        pgrad[at, SIDE:] = (hgrad * swish).astype(bf16)
        part = lax.dot_general(pgrad[at, :], win[...], COL_T, preferred_element_type=f32).astype(bf16)
        back[own, ROWS : 2 * ROWS, :] = part.reshape(group, ROWS, -1)
        return carry

    lax.fori_loop(0, COUNT // group, step, 0)
    for q in range(REP):
        x = rows[:, 0:ROWS, RI * q : RI * q + RI].reshape(COUNT * ROWS, RI)
        grad = lax.dot_general(x, pgrad[...], ROW_T, preferred_element_type=f32).astype(bf16)
        gpack[q, 0:RI, :] = grad[:, :SIDE]
        gpack[q, RI : 2 * RI, :] = grad[:, SIDE:]
    g = rows[:, ROWS : 2 * ROWS, :].reshape(COUNT * ROWS, -1)
    for j in range(3):
        gout[256 * j : 256 * j + 256, :] = lax.dot_general(
            hid[:, 256 * j : 256 * j + 256], g, ROW_T, preferred_element_type=f32
        ).astype(bf16)
    for q in range(REP):
        gpack[q, 2 * RI : 2 * RI + RO, :] = gout[RO * q : RO * q + RO, :SIDE]
        for i in range(3):
            gpack[q, 2 * RI + RO :, 256 * i : 256 * i + 256] = gout[RO * q + RT * i : RO * q + RT * i + RT, SIDE:]
    copies = [pltpu.make_async_copy(gpack.at[r], g0, gsem.at[0])]
    for s, t, b in ((2, g2t, g2b), (1, g1t, g1b), (3, g3t, g3b)):
        q = (r + s) % REP
        for out, at in ((t, 0), (b, HALF)):
            copies.append(pltpu.make_async_copy(gpack.at[q, at : at + HALF], out, gsem.at[len(copies)]))
    for c in copies:
        c.start()
    for c in copies:
        c.wait()


def expert(mine, rows, parts):
    width = rows.shape[2]
    piece = jax.ShapeDtypeStruct((SIDE, SIDE), bf16)
    half = jax.ShapeDtypeStruct((HALF, SIDE), bf16)
    total = COUNT * ROWS
    return pl.pallas_call(
        expert_body,
        out_shape=(jax.ShapeDtypeStruct(rows.shape, bf16), piece) + (half,) * 6,
        in_specs=[SMEM, VMEM] + [ANY] * 5,
        out_specs=(VMEM,) + (ANY,) * 7,
        scratch_shapes=[
            pltpu.VMEM((REP * RI, 2 * SIDE), bf16),
            pltpu.VMEM((REP * RO, width), bf16),
            pltpu.VMEM((total, SIDE), bf16),
            pltpu.VMEM((total, 2 * SIDE), bf16),
            pltpu.VMEM((SIDE, width), bf16),
            pltpu.VMEM((REP, SIDE, SIDE), bf16),
            pltpu.SemaphoreType.DMA((25,)),
            pltpu.SemaphoreType.DMA((2 * REP - 1,)),
        ],
        cost_estimate=pl.CostEstimate(flops=14_500_000_000, bytes_accessed=18_000_000, transcendentals=800_000),
        name="expert",
    )(mine, rows, *parts)


def adam(weight, gradient, first, second):
    first_new = beta_one * first + (1.0 - beta_one) * gradient
    second_new = beta_two * second + (1.0 - beta_two) * gradient * gradient
    ratio = (
        first_new
        / (1.0 - beta_one**steps_done)
        / (jnp.sqrt(second_new / (1.0 - beta_two**steps_done)) + epsilon)
    )
    master = weight.astype(f32)
    return (
        (master - learn_rate * (ratio + decay_rate * master)).astype(bf16),
        first_new,
        second_new,
    )


def update_body(w, moments, g0, g1t, g1b, g3t, g3b, w_in, w_out, f_in, s_in, f_out, s_out):
    def one(rows, lanes, outs, at, to):
        base = rows.start // HALF * HALF
        here = slice(rows.start - base, rows.stop - base)
        grad = g0[rows, lanes].astype(f32)
        for g in (g1b, g3b) if base else (g1t, g3t):
            grad = grad + g[here, lanes].astype(f32)
        second = slice(lanes.start + SIDE, lanes.stop + SIDE)
        new = adam(w[rows, lanes], grad, moments[rows, lanes].astype(f32), moments[rows, second].astype(f32))
        for o, v in zip(outs, new):
            o[at, to] = v

    ins = (w_in, f_in, s_in)
    outs = (w_out, f_out, s_out)
    whole = slice(0, SIDE)
    for i in range(RI // RT):
        here = slice(RT * i, RT * i + RT)
        one(here, whole, ins, here, whole)
        one(slice(RI + RT * i, RI + RT * i + RT), whole, ins, here, slice(SIDE, 2 * SIDE))
    for i in range(3):
        here = slice(RT * i, RT * i + RT)
        one(slice(2 * RI + RT * i, 2 * RI + RT * i + RT), whole, outs, here, whole)
        one(slice(2 * RI + RO, SIDE), slice(256 * i, 256 * i + 256), outs, here, slice(SIDE, SIDE + 256))


def update(w, moments, grads):
    return pl.pallas_call(
        update_body,
        out_shape=(
            jax.ShapeDtypeStruct((RI, 2 * SIDE), bf16),
            jax.ShapeDtypeStruct((RO, 1024), bf16),
            jax.ShapeDtypeStruct((RI, 2 * SIDE), f32),
            jax.ShapeDtypeStruct((RI, 2 * SIDE), f32),
            jax.ShapeDtypeStruct((RO, 1024), f32),
            jax.ShapeDtypeStruct((RO, 1024), f32),
        ),
        in_specs=[VMEM] * 7,
        out_specs=(VMEM,) * 6,
        name="update",
    )(w, moments, *grads)


def on_device(
    tokens,
    routes,
    gate_weights,
    cotangent,
    expert_plan,
    weight_in,
    weight_out,
    first_in,
    second_in,
    first_out,
    second_out,
):
    mine = lax.axis_index("dp").astype(jnp.int32).reshape(1)
    packed = pack(weight_in[0], weight_out[0], first_in[0], first_out[0], second_in[0], second_out[0])
    spread = exchange(packed.reshape(COUNT, SIDE // COUNT, 3 * SIDE))
    own = exchange(pick(expert_plan, spread, 2 * SIDE, SIDE)).reshape(SIDE, SIDE)
    outgoing, place, gated = dispatch(
        routes.transpose(2, 0, 1), gate_weights.transpose(2, 0, 1), expert_plan.reshape(-1, 1), tokens, cotangent
    )
    outgoing, own = lax.optimization_barrier((outgoing, own))
    before = shifted(own, 1)
    after = shifted(own, 3)
    top = shifted(before[:HALF], 1)
    bottom = shifted(after[HALF:], 3)
    parts = (own, before, top, bottom, after)
    arrived = exchange(outgoing)
    moved = pick(expert_plan, spread, 0, 2 * SIDE)
    arrived, moved = lax.optimization_barrier((arrived, moved))
    moments = exchange(moved).reshape(SIDE, 2 * SIDE)
    back, g0, g1t, g1b, g2t, g2b, g3t, g3b = expert(mine, arrived, parts)
    from_before = shifted(g2t, 1)
    from_after = shifted(g2b, 3)
    h1b = shifted(g1b, 1)
    h3t = shifted(g3t, 3)
    h1t = shifted(both(g1t, from_before), 1)
    h3b = shifted(both(g3b, from_after), 3)
    grads = (g0, h1t, h1b, h3t, h3b)
    returned = exchange(back)
    new_in, new_out, first_in_new, second_in_new, first_out_new, second_out_new = update(own, moments, grads)
    layer, token = combine(returned, place, gated)
    return (
        layer,
        token,
        new_in[None],
        new_out[None],
        first_in_new[None],
        second_in_new[None],
        first_out_new[None],
        second_out_new[None],
    )


def solution(mesh):
    rows = P(None, ("expert", "dp"), None)
    held = P("expert", "dp", None)
    return jax.shard_map(
        on_device,
        mesh=mesh,
        in_specs=(rows,) * 4 + (P(),) + (held,) * 6,
        out_specs=(rows,) * 2 + (held,) * 6,
        check_vma=False,
    )
```

```python
import jax
import jax.numpy as jnp
from jax import lax
from jax.experimental import pallas as pl
from jax.experimental.pallas import tpu as pltpu
from jax.sharding import PartitionSpec as P


beta_one = 0.9
beta_two = 0.95
learn_rate = 0.00042
decay_rate = 0.1
epsilon = 1e-08
steps_done = 10

SIDE = 768
RI = 256
RO = 192
RT = 64
REP = 4
COUNT = 32
CAP = 16
ROWS = 2 * CAP
HALF = SIDE // 2

f32 = jnp.float32
bf16 = jnp.bfloat16
VMEM = pl.BlockSpec(memory_space=pltpu.VMEM)
SMEM = pl.BlockSpec(memory_space=pltpu.SMEM)
ANY = pl.BlockSpec(memory_space=pl.ANY)


ROW_T = (((0,), (0,)), ((), ()))
COL_T = (((1,), (1,)), ((), ()))


def exchange(x):
    return lax.all_to_all(x, "expert", split_axis=0, concat_axis=0, tiled=True)


def shifted(x, by):
    return lax.ppermute(x, "dp", [(i, (i + by) % REP) for i in range(REP)])


def both(a, b):
    return (a.astype(f32) + b.astype(f32)).astype(bf16)


def pack_body(*refs):
    out = refs[-1]
    for j in range(len(refs) // 2):
        a, b = refs[2 * j : 2 * j + 2]
        lanes = slice(j * SIDE, (j + 1) * SIDE)
        out[0:RI, lanes] = a[:, :SIDE].astype(bf16)
        out[RI : 2 * RI, lanes] = a[:, SIDE:].astype(bf16)
        out[2 * RI : 2 * RI + RO, lanes] = b[:, :SIDE].astype(bf16)
        for i in range(3):
            at = j * SIDE + 256 * i
            out[2 * RI + RO :, at : at + 256] = b[RT * i : RT * i + RT, SIDE:].astype(bf16)


def pack(pairs, width):
    flat = [a for pair in pairs for a in pair]
    size = len(pairs) * SIDE
    return pl.pallas_call(
        pack_body,
        grid=(1,),
        out_shape=jax.ShapeDtypeStruct((SIDE, width), bf16),
        in_specs=[VMEM] * len(flat),
        out_specs=pl.BlockSpec((SIDE, size), lambda i: (0, 0)),
        name="pack",
    )(*flat)


def copy_picked(plan, src, out, lanes):
    def step(d, carry):
        out[d] = src[plan[d], :, lanes]
        return carry

    lax.fori_loop(0, COUNT, step, 0, unroll=True)


def pick_body(plan, src, out):
    copy_picked(plan, src, out, slice(0, out.shape[2]))


def pick(plan, src, size):
    return pl.pallas_call(
        pick_body,
        out_shape=jax.ShapeDtypeStruct(src.shape[:2] + (size,), bf16),
        in_specs=[SMEM, VMEM],
        out_specs=VMEM,
        compiler_params=pltpu.CompilerParams(vmem_limit_bytes=12 << 20),
        name="pick",
    )(plan, src)


def place_body(plan, src, held, out):
    copy_picked(plan, src, out, slice(0, SIDE))


def place_picked(plan, src, held):
    return pl.pallas_call(
        place_body,
        grid=(1,),
        out_shape=jax.ShapeDtypeStruct(held.shape, bf16),
        in_specs=[SMEM, VMEM, pl.BlockSpec(memory_space=pltpu.HBM)],
        out_specs=pl.BlockSpec(src.shape, lambda i: (0, 0, 2)),
        input_output_aliases={2: 0},
        compiler_params=pltpu.CompilerParams(vmem_limit_bytes=50 << 20),
        name="place",
    )(plan, src, held)


def dispatch_body(routes, gates, plan, tokens, cotangent, out, place, gated):
    n = tokens.shape[1]
    top = routes.shape[0]
    holder = plan[...]
    earlier = (
        lax.broadcasted_iota(jnp.int32, (n, n), 0) < lax.broadcasted_iota(jnp.int32, (n, n), 1)
    ).astype(bf16)
    same = (
        lax.broadcasted_iota(jnp.int32, (n, n), 0) == lax.broadcasted_iota(jnp.int32, (n, n), 1)
    ).astype(bf16)
    slot = lax.broadcasted_iota(jnp.int32, (COUNT, CAP, n), 1).astype(f32)
    for m in range(2):
        hit = jnp.zeros((COUNT, n), f32)
        gate = jnp.zeros((COUNT, n), f32)
        for k in range(top):
            one = routes[k, m : m + 1, :] == holder
            hit = hit + jnp.where(one, 1.0, 0.0)
            gate = gate + jnp.where(one, gates[k, m : m + 1, :], 0.0)
        rank = jnp.dot(hit.astype(bf16), earlier, preferred_element_type=f32)
        rank = jnp.where(hit > 0.0, rank, -1.0)
        wide = jnp.broadcast_to(rank[:, None, :], (COUNT, CAP, n))
        chosen = jnp.where(wide == slot, 1.0, 0.0)
        weighted = chosen * jnp.broadcast_to(gate[:, None, :], (COUNT, CAP, n))
        chosen = chosen.reshape(COUNT * CAP, n)
        weighted = weighted.reshape(COUNT * CAP, n)
        column = jnp.sum(weighted, axis=1, keepdims=True)
        chosen = chosen.astype(bf16)
        high = weighted.astype(bf16)
        low = (weighted - high.astype(f32)).astype(bf16)
        place[m] = lax.dot_general(same, chosen, COL_T, preferred_element_type=f32).astype(bf16)
        gated[m, :n] = lax.dot_general(same, high, COL_T, preferred_element_type=f32).astype(bf16)
        gated[m, n:] = lax.dot_general(same, low, COL_T, preferred_element_type=f32).astype(bf16)
        sent = jnp.dot(chosen, tokens[m], preferred_element_type=f32).astype(bf16)
        out[:, CAP * m : CAP * m + CAP, :] = sent.reshape(COUNT, CAP, -1)
        grads = jnp.dot(chosen, cotangent[m], preferred_element_type=f32) * column
        out[:, ROWS + CAP * m : ROWS + CAP * m + CAP, :] = grads.astype(bf16).reshape(COUNT, CAP, -1)


def dispatch(routes, gates, plan, tokens, cotangent):
    n, width = tokens.shape[1:]
    return pl.pallas_call(
        dispatch_body,
        out_shape=(
            jax.ShapeDtypeStruct((COUNT, 2 * ROWS, width), bf16),
            jax.ShapeDtypeStruct((2, n, COUNT * CAP), bf16),
            jax.ShapeDtypeStruct((2, 2 * n, COUNT * CAP), bf16),
        ),
        in_specs=[VMEM] * 5,
        out_specs=(VMEM, VMEM, VMEM),
        name="dispatch",
    )(routes, gates, plan, tokens, cotangent)


def combine_body(back, place, gated, layer, token):
    n = layer.shape[1]
    for m in range(2):
        rows = back[:, CAP * m : CAP * m + CAP, :].reshape(COUNT * CAP, -1)
        sums = jnp.dot(gated[m], rows, preferred_element_type=f32)
        layer[m] = (sums[:n] + sums[n:]).astype(bf16)
        rows = back[:, ROWS + CAP * m : ROWS + CAP * m + CAP, :].reshape(COUNT * CAP, -1)
        token[m] = jnp.dot(place[m], rows, preferred_element_type=f32).astype(bf16)


def combine(back, place, gated):
    n = place.shape[1]
    width = back.shape[2]
    shape = jax.ShapeDtypeStruct((2, n, width), bf16)
    return pl.pallas_call(
        combine_body,
        out_shape=(shape, shape),
        in_specs=[VMEM] * 3,
        out_specs=(VMEM, VMEM),
        name="combine",
    )(back, place, gated)


def expert_body(mine, rows, w0, w1, w2a, w2b, w3, back, g0, g1t, g1b, g2t, g2b, g3t, g3b, win, wout, hid, pgrad, gout, gpack, sem, gsem):
    r = mine[0]
    copies = []

    def fetch(s, w, lo, hi, src):
        q = (r - s + REP) % REP
        at = pl.multiple_of(q * RI, RI)
        to = pl.multiple_of(q * RO, RT)
        pieces = []
        for base, end, ref, first, lanes in (
            (0, RI, win, at, 0),
            (RI, 2 * RI, win, at, SIDE),
            (2 * RI, 2 * RI + RO, wout, to, 0),
        ):
            l, h = max(lo, base), min(hi, end)
            if l < h:
                start = pl.multiple_of(first + (l - base), RT)
                pieces.append((w.at[l - lo + src : h - lo + src], ref.at[pl.ds(start, h - l), lanes : lanes + SIDE]))
        if hi == SIDE:
            for i in range(3):
                l = 2 * RI + RO - lo + src
                start = pl.multiple_of(to + RT * i, RT)
                pieces.append(
                    (w.at[l : l + RT, 256 * i : 256 * i + 256], wout.at[pl.ds(start, RT), SIDE : SIDE + 256])
                )
        for x, y in pieces:
            copies.append(pltpu.make_async_copy(x, y, sem.at[len(copies)]))

    fetch(0, w0, 0, SIDE, 0)
    fetch(1, w1, 0, SIDE, 0)
    fetch(2, w2a, 0, HALF, 0)
    fetch(2, w2b, HALF, SIDE, 0)
    fetch(3, w3, 0, SIDE, 0)
    for c in copies:
        c.start()
    for c in copies:
        c.wait()

    group = 8
    size = group * ROWS

    def step(i, carry):
        own = pl.ds(pl.multiple_of(i * group, group), group)
        at = pl.ds(pl.multiple_of(i * size, size), size)
        x = rows[own, 0:ROWS, :].reshape(size, -1)
        pre = jnp.dot(x, win[...], preferred_element_type=f32)
        gate = pre[:, :SIDE]
        up = pre[:, SIDE:]
        sigma = jax.nn.sigmoid(gate)
        swish = gate * sigma
        hidden = (swish * up).astype(bf16)
        hid[at, :] = hidden
        out = jnp.dot(hidden, wout[...], preferred_element_type=f32).astype(bf16)
        back[own, 0:ROWS, :] = out.reshape(group, ROWS, -1)
        g = rows[own, ROWS : 2 * ROWS, :].reshape(size, -1)
        hgrad = lax.dot_general(g, wout[...], COL_T, preferred_element_type=f32)
        pgrad[at, 0:SIDE] = (hgrad * up * sigma * (1.0 + gate * (1.0 - sigma))).astype(bf16)
        pgrad[at, SIDE:] = (hgrad * swish).astype(bf16)
        part = lax.dot_general(pgrad[at, :], win[...], COL_T, preferred_element_type=f32).astype(bf16)
        back[own, ROWS : 2 * ROWS, :] = part.reshape(group, ROWS, -1)
        return carry

    lax.fori_loop(0, COUNT // group, step, 0)
    for q in range(REP):
        x = rows[:, 0:ROWS, RI * q : RI * q + RI].reshape(COUNT * ROWS, RI)
        grad = lax.dot_general(x, pgrad[...], ROW_T, preferred_element_type=f32).astype(bf16)
        gpack[q, 0:RI, :] = grad[:, :SIDE]
        gpack[q, RI : 2 * RI, :] = grad[:, SIDE:]
    g = rows[:, ROWS : 2 * ROWS, :].reshape(COUNT * ROWS, -1)
    for j in range(3):
        gout[256 * j : 256 * j + 256, :] = lax.dot_general(
            hid[:, 256 * j : 256 * j + 256], g, ROW_T, preferred_element_type=f32
        ).astype(bf16)
    for q in range(REP):
        gpack[q, 2 * RI : 2 * RI + RO, :] = gout[RO * q : RO * q + RO, :SIDE]
        for i in range(3):
            gpack[q, 2 * RI + RO :, 256 * i : 256 * i + 256] = gout[RO * q + RT * i : RO * q + RT * i + RT, SIDE:]
    copies = [pltpu.make_async_copy(gpack.at[r], g0, gsem.at[0])]
    for s, t, b in ((2, g2t, g2b), (1, g1t, g1b), (3, g3t, g3b)):
        q = (r + s) % REP
        for out, at in ((t, 0), (b, HALF)):
            copies.append(pltpu.make_async_copy(gpack.at[q, at : at + HALF], out, gsem.at[len(copies)]))
    for c in copies:
        c.start()
    for c in copies:
        c.wait()


def expert(mine, rows, parts):
    width = rows.shape[2]
    piece = jax.ShapeDtypeStruct((SIDE, SIDE), bf16)
    half = jax.ShapeDtypeStruct((HALF, SIDE), bf16)
    total = COUNT * ROWS
    return pl.pallas_call(
        expert_body,
        out_shape=(jax.ShapeDtypeStruct(rows.shape, bf16), piece) + (half,) * 6,
        in_specs=[SMEM, VMEM] + [ANY] * 5,
        out_specs=(VMEM,) + (ANY,) * 7,
        scratch_shapes=[
            pltpu.VMEM((REP * RI, 2 * SIDE), bf16),
            pltpu.VMEM((REP * RO, width), bf16),
            pltpu.VMEM((total, SIDE), bf16),
            pltpu.VMEM((total, 2 * SIDE), bf16),
            pltpu.VMEM((SIDE, width), bf16),
            pltpu.VMEM((REP, SIDE, SIDE), bf16),
            pltpu.SemaphoreType.DMA((25,)),
            pltpu.SemaphoreType.DMA((2 * REP - 1,)),
        ],
        cost_estimate=pl.CostEstimate(flops=14_500_000_000, bytes_accessed=18_000_000, transcendentals=800_000),
        name="expert",
    )(mine, rows, *parts)


def adam(weight, gradient, first, second):
    first_new = beta_one * first + (1.0 - beta_one) * gradient
    second_new = beta_two * second + (1.0 - beta_two) * gradient * gradient
    ratio = (
        first_new
        / (1.0 - beta_one**steps_done)
        / (jnp.sqrt(second_new / (1.0 - beta_two**steps_done)) + epsilon)
    )
    master = weight.astype(f32)
    return (
        (master - learn_rate * (ratio + decay_rate * master)).astype(bf16),
        first_new,
        second_new,
    )


def update_body(w, moments, g0, g1t, g1b, g3t, g3b, w_in, w_out, f_in, s_in, f_out, s_out):
    def one(rows, lanes, outs, at, to):
        base = rows.start // HALF * HALF
        here = slice(rows.start - base, rows.stop - base)
        grad = g0[rows, lanes].astype(f32)
        for g in (g1b, g3b) if base else (g1t, g3t):
            grad = grad + g[here, lanes].astype(f32)
        second = slice(lanes.start + SIDE, lanes.stop + SIDE)
        new = adam(w[rows, lanes], grad, moments[rows, lanes].astype(f32), moments[rows, second].astype(f32))
        for o, v in zip(outs, new):
            o[at, to] = v

    ins = (w_in, f_in, s_in)
    outs = (w_out, f_out, s_out)
    whole = slice(0, SIDE)
    for i in range(RI // RT):
        here = slice(RT * i, RT * i + RT)
        one(here, whole, ins, here, whole)
        one(slice(RI + RT * i, RI + RT * i + RT), whole, ins, here, slice(SIDE, 2 * SIDE))
    for i in range(3):
        here = slice(RT * i, RT * i + RT)
        one(slice(2 * RI + RT * i, 2 * RI + RT * i + RT), whole, outs, here, whole)
        one(slice(2 * RI + RO, SIDE), slice(256 * i, 256 * i + 256), outs, here, slice(SIDE, SIDE + 256))


def update(w, moments, grads):
    return pl.pallas_call(
        update_body,
        out_shape=(
            jax.ShapeDtypeStruct((RI, 2 * SIDE), bf16),
            jax.ShapeDtypeStruct((RO, 1024), bf16),
            jax.ShapeDtypeStruct((RI, 2 * SIDE), f32),
            jax.ShapeDtypeStruct((RI, 2 * SIDE), f32),
            jax.ShapeDtypeStruct((RO, 1024), f32),
            jax.ShapeDtypeStruct((RO, 1024), f32),
        ),
        in_specs=[VMEM] * 7,
        out_specs=(VMEM,) * 6,
        compiler_params=pltpu.CompilerParams(vmem_limit_bytes=32 << 20),
        name="update",
    )(w, moments, *grads)


def on_device(
    tokens,
    routes,
    gate_weights,
    cotangent,
    expert_plan,
    weight_in,
    weight_out,
    first_in,
    second_in,
    first_out,
    second_out,
):
    mine = lax.axis_index("dp").astype(jnp.int32).reshape(1)
    slim = (COUNT, SIDE // COUNT, SIDE)
    wide = (COUNT, SIDE // COUNT, 3 * SIDE)
    weights = exchange(pack(((weight_in[0], weight_out[0]),), SIDE).reshape(slim))
    held = pack(((first_in[0], first_out[0]), (second_in[0], second_out[0])), 3 * SIDE)
    filled = place_picked(expert_plan, weights, held.reshape(wide))
    spread = exchange(filled)
    own = spread[:, :, 2 * SIDE :].reshape(SIDE, SIDE)
    outgoing, place, gated = dispatch(
        routes.transpose(2, 0, 1), gate_weights.transpose(2, 0, 1), expert_plan.reshape(-1, 1), tokens, cotangent
    )
    before = shifted(own, 1)
    after = shifted(own, 3)
    top = shifted(before[:HALF], 1)
    bottom = shifted(after[HALF:], 3)
    parts = (own, before, top, bottom, after)
    arrived = exchange(outgoing)
    moved = pick(expert_plan, spread, 2 * SIDE)
    moments = exchange(moved).reshape(SIDE, 2 * SIDE)
    back, g0, g1t, g1b, g2t, g2b, g3t, g3b = expert(mine, arrived, parts)
    from_before = shifted(g2t, 1)
    from_after = shifted(g2b, 3)
    h1b = shifted(g1b, 1)
    h3t = shifted(g3t, 3)
    h1t = shifted(both(g1t, from_before), 1)
    h3b = shifted(both(g3b, from_after), 3)
    grads = (g0, h1t, h1b, h3t, h3b)
    returned = exchange(back)
    new_in, new_out, first_in_new, second_in_new, first_out_new, second_out_new = update(own, moments, grads)
    layer, token = combine(returned, place, gated)
    return (
        layer,
        token,
        new_in[None],
        new_out[None],
        first_in_new[None],
        second_in_new[None],
        first_out_new[None],
        second_out_new[None],
    )


def solution(mesh):
    rows = P(None, ("expert", "dp"), None)
    held = P("expert", "dp", None)
    return jax.shard_map(
        on_device,
        mesh=mesh,
        in_specs=(rows,) * 4 + (P(),) + (held,) * 6,
        out_specs=(rows,) * 2 + (held,) * 6,
        check_vma=False,
    )
```

```python
import jax
import jax.numpy as jnp
from jax import lax
from jax.experimental import pallas as pl
from jax.experimental.pallas import tpu as pltpu
from jax.sharding import PartitionSpec as P


beta_one = 0.9
beta_two = 0.95
learn_rate = 0.00042
decay_rate = 0.1
epsilon = 1e-08
steps_done = 10

SIDE = 768
RI = 256
RO = 192
RT = 64
REP = 4
COUNT = 32
CAP = 16
ROWS = 2 * CAP
HALF = SIDE // 2

f32 = jnp.float32
bf16 = jnp.bfloat16
VMEM = pl.BlockSpec(memory_space=pltpu.VMEM)
SMEM = pl.BlockSpec(memory_space=pltpu.SMEM)
ANY = pl.BlockSpec(memory_space=pl.ANY)


ROW_T = (((0,), (0,)), ((), ()))
COL_T = (((1,), (1,)), ((), ()))


def exchange(x):
    return lax.all_to_all(x, "expert", split_axis=0, concat_axis=0, tiled=True)


def shifted(x, by):
    return lax.ppermute(x, "dp", [(i, (i + by) % REP) for i in range(REP)])


def along_first(x, s):
    return lax.ppermute(x, "expert", [(i, (i + 8 * s) % COUNT) for i in range(COUNT)])


def along_second(x, t):
    return lax.ppermute(x, "expert", [(i, i // 8 * 8 + (i + 2 * t) % 8) for i in range(COUNT)])


def along_third(x):
    return lax.ppermute(x, "expert", [(i, i ^ 1) for i in range(COUNT)])


def spread_offsets(x):
    first = x[..., :SIDE]
    second = x[..., SIDE:]
    a = [first[0]] + [along_first(first[s], s) for s in range(1, 4)]
    b = [second[:, 0]] + [along_second(second[:, t], t) for t in range(1, 4)]
    a = [jnp.stack([g[t] for g in a]) for t in range(4)]
    b = [jnp.stack([g[s] for g in b]) for s in range(4)]
    a = jnp.stack([a[0]] + [along_second(a[t], t) for t in range(1, 4)])
    b = jnp.stack([b[0]] + [along_first(b[s], s) for s in range(1, 4)], axis=1)
    done = jnp.concatenate([a, b], axis=-1)
    other = along_third(done[:, :, 1])
    return jnp.concatenate([done[:, :, 0], other], axis=0).reshape(COUNT, *x.shape[3:])


def both(a, b):
    return (a.astype(f32) + b.astype(f32)).astype(bf16)


def pack_body(*refs):
    out = refs[-1]
    for j in range(len(refs) // 2):
        a, b = refs[2 * j : 2 * j + 2]
        lanes = slice(j * SIDE, (j + 1) * SIDE)
        out[0:RI, lanes] = a[:, :SIDE].astype(bf16)
        out[RI : 2 * RI, lanes] = a[:, SIDE:].astype(bf16)
        out[2 * RI : 2 * RI + RO, lanes] = b[:, :SIDE].astype(bf16)
        for i in range(3):
            at = j * SIDE + 256 * i
            out[2 * RI + RO :, at : at + 256] = b[RT * i : RT * i + RT, SIDE:].astype(bf16)


def pack(pairs, width):
    flat = [a for pair in pairs for a in pair]
    size = len(pairs) * SIDE
    return pl.pallas_call(
        pack_body,
        grid=(1,),
        out_shape=jax.ShapeDtypeStruct((SIDE, width), bf16),
        in_specs=[VMEM] * len(flat),
        out_specs=pl.BlockSpec((SIDE, size), lambda i: (0, 0)),
        name="pack",
    )(*flat)


def copy_picked(plan, src, out, lanes):
    def step(d, carry):
        out[d] = src[plan[d], :, lanes]
        return carry

    lax.fori_loop(0, COUNT, step, 0, unroll=True)


def pick_body(plan, src, out):
    copy_picked(plan, src, out, slice(0, out.shape[2]))


def pick(plan, src, size):
    return pl.pallas_call(
        pick_body,
        out_shape=jax.ShapeDtypeStruct(src.shape[:2] + (size,), bf16),
        in_specs=[SMEM, VMEM],
        out_specs=VMEM,
        compiler_params=pltpu.CompilerParams(vmem_limit_bytes=12 << 20),
        name="pick",
    )(plan, src)


def dispatch_body(routes, gates, plan, tokens, cotangent, out, place, gated):
    n = tokens.shape[1]
    top = routes.shape[0]
    holder = plan[...]
    earlier = (
        lax.broadcasted_iota(jnp.int32, (n, n), 0) < lax.broadcasted_iota(jnp.int32, (n, n), 1)
    ).astype(bf16)
    same = (
        lax.broadcasted_iota(jnp.int32, (n, n), 0) == lax.broadcasted_iota(jnp.int32, (n, n), 1)
    ).astype(bf16)
    slot = lax.broadcasted_iota(jnp.int32, (COUNT, CAP, n), 1).astype(f32)
    for m in range(2):
        hit = jnp.zeros((COUNT, n), f32)
        gate = jnp.zeros((COUNT, n), f32)
        for k in range(top):
            one = routes[k, m : m + 1, :] == holder
            hit = hit + jnp.where(one, 1.0, 0.0)
            gate = gate + jnp.where(one, gates[k, m : m + 1, :], 0.0)
        rank = jnp.dot(hit.astype(bf16), earlier, preferred_element_type=f32)
        rank = jnp.where(hit > 0.0, rank, -1.0)
        wide = jnp.broadcast_to(rank[:, None, :], (COUNT, CAP, n))
        chosen = jnp.where(wide == slot, 1.0, 0.0)
        weighted = chosen * jnp.broadcast_to(gate[:, None, :], (COUNT, CAP, n))
        chosen = chosen.reshape(COUNT * CAP, n)
        weighted = weighted.reshape(COUNT * CAP, n)
        column = jnp.sum(weighted, axis=1, keepdims=True)
        chosen = chosen.astype(bf16)
        high = weighted.astype(bf16)
        low = (weighted - high.astype(f32)).astype(bf16)
        place[m] = lax.dot_general(same, chosen, COL_T, preferred_element_type=f32).astype(bf16)
        gated[m, :n] = lax.dot_general(same, high, COL_T, preferred_element_type=f32).astype(bf16)
        gated[m, n:] = lax.dot_general(same, low, COL_T, preferred_element_type=f32).astype(bf16)
        sent = jnp.dot(chosen, tokens[m], preferred_element_type=f32).astype(bf16)
        out[:, CAP * m : CAP * m + CAP, :] = sent.reshape(COUNT, CAP, -1)
        grads = jnp.dot(chosen, cotangent[m], preferred_element_type=f32) * column
        out[:, ROWS + CAP * m : ROWS + CAP * m + CAP, :] = grads.astype(bf16).reshape(COUNT, CAP, -1)


def dispatch(routes, gates, plan, tokens, cotangent):
    n, width = tokens.shape[1:]
    return pl.pallas_call(
        dispatch_body,
        out_shape=(
            jax.ShapeDtypeStruct((COUNT, 2 * ROWS, width), bf16),
            jax.ShapeDtypeStruct((2, n, COUNT * CAP), bf16),
            jax.ShapeDtypeStruct((2, 2 * n, COUNT * CAP), bf16),
        ),
        in_specs=[VMEM] * 5,
        out_specs=(VMEM, VMEM, VMEM),
        name="dispatch",
    )(routes, gates, plan, tokens, cotangent)


def combine_body(back, place, gated, layer, token):
    n = layer.shape[1]
    for m in range(2):
        rows = back[:, CAP * m : CAP * m + CAP, :].reshape(COUNT * CAP, -1)
        sums = jnp.dot(gated[m], rows, preferred_element_type=f32)
        layer[m] = (sums[:n] + sums[n:]).astype(bf16)
        rows = back[:, ROWS + CAP * m : ROWS + CAP * m + CAP, :].reshape(COUNT * CAP, -1)
        token[m] = jnp.dot(place[m], rows, preferred_element_type=f32).astype(bf16)


def combine(back, place, gated):
    n = place.shape[1]
    width = back.shape[2]
    shape = jax.ShapeDtypeStruct((2, n, width), bf16)
    return pl.pallas_call(
        combine_body,
        out_shape=(shape, shape),
        in_specs=[VMEM] * 3,
        out_specs=(VMEM, VMEM),
        name="combine",
    )(back, place, gated)


def expert_body(mine, sent, w0, w1, w2, w3, given, g0, g1t, g1b, g2t, g2b, g3t, g3b, win, wout, hid, pgrad, gout, gpack, rows, back, sem, gsem, rsem, bsem):
    r = mine[0]
    copies = []

    def fetch(s, w, lo, hi, src):
        q = (r - s + REP) % REP
        at = pl.multiple_of(q * RI, RI)
        to = pl.multiple_of(q * RO, RT)
        pieces = []
        for base, end, ref, first, lanes in (
            (0, RI, win, at, 0),
            (RI, 2 * RI, win, at, SIDE),
            (2 * RI, 2 * RI + RO, wout, to, 0),
        ):
            l, h = max(lo, base), min(hi, end)
            if l < h:
                start = pl.multiple_of(first + (l - base), RT)
                pieces.append((w.at[l - lo + src : h - lo + src], ref.at[pl.ds(start, h - l), lanes : lanes + SIDE]))
        if hi == SIDE:
            for i in range(3):
                l = 2 * RI + RO - lo + src
                start = pl.multiple_of(to + RT * i, RT)
                pieces.append(
                    (w.at[l : l + RT, 256 * i : 256 * i + 256], wout.at[pl.ds(start, RT), SIDE : SIDE + 256])
                )
        for x, y in pieces:
            copies.append(pltpu.make_async_copy(x, y, sem.at[len(copies)]))

    fetch(0, w0, 0, SIDE, 0)
    fetch(1, w1, 0, SIDE, 0)
    fetch(2, w2, 0, SIDE, 0)
    fetch(3, w3, 0, SIDE, 0)
    group = 8
    size = group * ROWS

    def incoming(i):
        own = pl.ds(i * group, group)
        return pltpu.make_async_copy(sent.at[own], rows.at[own], rsem.at[i])

    def outgoing(i):
        own = pl.ds(i * group, group)
        return pltpu.make_async_copy(back.at[own], given.at[own], bsem.at[i])

    blocks = COUNT // group
    incoming(0).start()
    for c in copies:
        c.start()
    for i in range(1, blocks):
        incoming(i).start()
    for c in copies:
        c.wait()

    def step(i, carry):
        incoming(i).wait()
        own = pl.ds(pl.multiple_of(i * group, group), group)
        at = pl.ds(pl.multiple_of(i * size, size), size)
        x = rows[own, 0:ROWS, :].reshape(size, -1)
        pre = jnp.dot(x, win[...], preferred_element_type=f32)
        gate = pre[:, :SIDE]
        up = pre[:, SIDE:]
        sigma = jax.nn.sigmoid(gate)
        swish = gate * sigma
        hidden = (swish * up).astype(bf16)
        hid[at, :] = hidden
        out = jnp.dot(hidden, wout[...], preferred_element_type=f32).astype(bf16)
        back[own, 0:ROWS, :] = out.reshape(group, ROWS, -1)
        g = rows[own, ROWS : 2 * ROWS, :].reshape(size, -1)
        hgrad = lax.dot_general(g, wout[...], COL_T, preferred_element_type=f32)
        pgrad[at, 0:SIDE] = (hgrad * up * sigma * (1.0 + gate * (1.0 - sigma))).astype(bf16)
        pgrad[at, SIDE:] = (hgrad * swish).astype(bf16)
        part = lax.dot_general(pgrad[at, :], win[...], COL_T, preferred_element_type=f32).astype(bf16)
        back[own, ROWS : 2 * ROWS, :] = part.reshape(group, ROWS, -1)
        outgoing(i).start()
        return carry

    lax.fori_loop(0, blocks, step, 0)
    for q in range(REP):
        x = rows[:, 0:ROWS, RI * q : RI * q + RI].reshape(COUNT * ROWS, RI)
        grad = lax.dot_general(x, pgrad[...], ROW_T, preferred_element_type=f32).astype(bf16)
        gpack[q, 0:RI, :] = grad[:, :SIDE]
        gpack[q, RI : 2 * RI, :] = grad[:, SIDE:]
    g = rows[:, ROWS : 2 * ROWS, :].reshape(COUNT * ROWS, -1)
    for j in range(3):
        gout[256 * j : 256 * j + 256, :] = lax.dot_general(
            hid[:, 256 * j : 256 * j + 256], g, ROW_T, preferred_element_type=f32
        ).astype(bf16)
    for q in range(REP):
        gpack[q, 2 * RI : 2 * RI + RO, :] = gout[RO * q : RO * q + RO, :SIDE]
        for i in range(3):
            gpack[q, 2 * RI + RO :, 256 * i : 256 * i + 256] = gout[RO * q + RT * i : RO * q + RT * i + RT, SIDE:]
    copies = [pltpu.make_async_copy(gpack.at[r], g0, gsem.at[0])]
    for s, t, b in ((2, g2t, g2b), (1, g1t, g1b), (3, g3t, g3b)):
        q = (r + s) % REP
        for out, at in ((t, 0), (b, HALF)):
            copies.append(pltpu.make_async_copy(gpack.at[q, at : at + HALF], out, gsem.at[len(copies)]))
    for c in copies:
        c.start()
    for i in range(blocks):
        outgoing(i).wait()
    for c in copies:
        c.wait()


def expert(mine, rows, parts):
    width = rows.shape[2]
    piece = jax.ShapeDtypeStruct((SIDE, SIDE), bf16)
    half = jax.ShapeDtypeStruct((HALF, SIDE), bf16)
    total = COUNT * ROWS
    return pl.pallas_call(
        expert_body,
        out_shape=(jax.ShapeDtypeStruct(rows.shape, bf16), piece) + (half,) * 6,
        in_specs=[SMEM] + [ANY] * 5,
        out_specs=(ANY,) * 8,
        scratch_shapes=[
            pltpu.VMEM((REP * RI, 2 * SIDE), bf16),
            pltpu.VMEM((REP * RO, width), bf16),
            pltpu.VMEM((total, SIDE), bf16),
            pltpu.VMEM((total, 2 * SIDE), bf16),
            pltpu.VMEM((SIDE, width), bf16),
            pltpu.VMEM((REP, SIDE, SIDE), bf16),
            pltpu.VMEM(rows.shape, bf16),
            pltpu.VMEM(rows.shape, bf16),
            pltpu.SemaphoreType.DMA((24,)),
            pltpu.SemaphoreType.DMA((2 * REP - 1,)),
            pltpu.SemaphoreType.DMA((4,)),
            pltpu.SemaphoreType.DMA((4,)),
        ],
        cost_estimate=pl.CostEstimate(flops=14_500_000_000, bytes_accessed=18_000_000, transcendentals=800_000),
        name="expert",
    )(mine, rows, *parts)


def adam(weight, gradient, first, second):
    first_new = beta_one * first + (1.0 - beta_one) * gradient
    second_new = beta_two * second + (1.0 - beta_two) * gradient * gradient
    ratio = (
        first_new
        / (1.0 - beta_one**steps_done)
        / (jnp.sqrt(second_new / (1.0 - beta_two**steps_done)) + epsilon)
    )
    master = weight.astype(f32)
    return (
        (master - learn_rate * (ratio + decay_rate * master)).astype(bf16),
        first_new,
        second_new,
    )


def update_body(w, moments, g0, g1t, g1b, g3t, g3b, w_in, w_out, f_in, s_in, f_out, s_out):
    def one(rows, lanes, outs, at, to):
        base = rows.start // HALF * HALF
        here = slice(rows.start - base, rows.stop - base)
        grad = g0[rows, lanes].astype(f32)
        for g in (g1b, g3b) if base else (g1t, g3t):
            grad = grad + g[here, lanes].astype(f32)
        second = slice(lanes.start + SIDE, lanes.stop + SIDE)
        new = adam(w[rows, lanes], grad, moments[rows, lanes].astype(f32), moments[rows, second].astype(f32))
        for o, v in zip(outs, new):
            o[at, to] = v

    ins = (w_in, f_in, s_in)
    outs = (w_out, f_out, s_out)
    whole = slice(0, SIDE)
    for i in range(RI // RT):
        here = slice(RT * i, RT * i + RT)
        one(here, whole, ins, here, whole)
        one(slice(RI + RT * i, RI + RT * i + RT), whole, ins, here, slice(SIDE, 2 * SIDE))
    for i in range(3):
        here = slice(RT * i, RT * i + RT)
        one(slice(2 * RI + RT * i, 2 * RI + RT * i + RT), whole, outs, here, whole)
        one(slice(2 * RI + RO, SIDE), slice(256 * i, 256 * i + 256), outs, here, slice(SIDE, SIDE + 256))


def update(w, moments, grads):
    return pl.pallas_call(
        update_body,
        out_shape=(
            jax.ShapeDtypeStruct((RI, 2 * SIDE), bf16),
            jax.ShapeDtypeStruct((RO, 1024), bf16),
            jax.ShapeDtypeStruct((RI, 2 * SIDE), f32),
            jax.ShapeDtypeStruct((RI, 2 * SIDE), f32),
            jax.ShapeDtypeStruct((RO, 1024), f32),
            jax.ShapeDtypeStruct((RO, 1024), f32),
        ),
        in_specs=[VMEM] * 7,
        out_specs=(VMEM,) * 6,
        compiler_params=pltpu.CompilerParams(vmem_limit_bytes=32 << 20),
        name="update",
    )(w, moments, *grads)


def on_device(
    tokens,
    routes,
    gate_weights,
    cotangent,
    expert_plan,
    weight_in,
    weight_out,
    first_in,
    second_in,
    first_out,
    second_out,
):
    mine = lax.axis_index("dp").astype(jnp.int32).reshape(1)
    slim = (COUNT, SIDE // COUNT, SIDE)
    weights = exchange(pack(((weight_in[0], weight_out[0]),), SIDE).reshape(slim))
    held = pack(((first_in[0], first_out[0]), (second_in[0], second_out[0])), 2 * SIDE)
    spread = spread_offsets(held.reshape(4, 4, 2, SIDE // COUNT, 2 * SIDE))
    here = lax.axis_index("expert").astype(jnp.int32)
    each = jnp.arange(COUNT, dtype=jnp.int32)
    source = (here + expert_plan) % 2 * 16 + (here // 2 - expert_plan // 2) % 4 * 4 + (here // 8 - expert_plan // 8) % 4
    held_here = jnp.sum(jnp.where(each == here, expert_plan, 0))
    holder = (
        (held_here // 8 + each // 8) % 4 * 8 + (held_here // 2 + each // 2) % 4 * 2 + (held_here + each) % 2
    )
    picked = pick(expert_plan, weights, SIDE)
    own = exchange(picked).reshape(SIDE, SIDE)
    outgoing, place, gated = dispatch(
        routes.transpose(2, 0, 1), gate_weights.transpose(2, 0, 1), expert_plan.reshape(-1, 1), tokens, cotangent
    )
    parts = (own,) + tuple(shifted(own, r) for r in range(1, REP))
    arrived = exchange(outgoing)
    moved = pick(source, spread, 2 * SIDE)
    landed = exchange(moved)
    moments = pick(holder, landed, 2 * SIDE).reshape(SIDE, 2 * SIDE)
    back, g0, g1t, g1b, g2t, g2b, g3t, g3b = expert(mine, arrived, parts)
    from_before = shifted(g2t, 1)
    from_after = shifted(g2b, 3)
    h1b = shifted(g1b, 1)
    h3t = shifted(g3t, 3)
    h1t = shifted(both(g1t, from_before), 1)
    h3b = shifted(both(g3b, from_after), 3)
    grads = (g0, h1t, h1b, h3t, h3b)
    returned = exchange(back)
    new_in, new_out, first_in_new, second_in_new, first_out_new, second_out_new = update(own, moments, grads)
    layer, token = combine(returned, place, gated)
    return (
        layer,
        token,
        new_in[None],
        new_out[None],
        first_in_new[None],
        second_in_new[None],
        first_out_new[None],
        second_out_new[None],
    )


def solution(mesh):
    rows = P(None, ("expert", "dp"), None)
    held = P("expert", "dp", None)
    return jax.shard_map(
        on_device,
        mesh=mesh,
        in_specs=(rows,) * 4 + (P(),) + (held,) * 6,
        out_specs=(rows,) * 2 + (held,) * 6,
        check_vma=False,
    )
```
